32 devices in a mesh: rows: 4 (over y, core), cols: 8 (over z, x).
Axes of the slice: x: 2, y: 2, z: 4, core: 2. Of those that a mesh axis runs over, the one named last changes fastest.
Arguments:
- single: bfloat16 [512, 1024], P('rows'), may hold values from -6 to 6
- pair: bfloat16 [512, 512, 128], P('rows', 'cols'), may hold values from -6 to 6
- residue_mask: int32 [512], replicated, may hold values from 0 to 1, as said below
- w_bias: bfloat16 [128, 32], replicated, may hold values from -40 to 40
- w_project: bfloat16 [4, 1024, 1024], P(None, None, 'cols'), may hold values from -0.1875 to 0.1875
- w_out: bfloat16 [1024, 1024], replicated, may hold values from -0.1875 to 0.1875
- w_factors: bfloat16 [1024, 128], replicated, may hold values from -0.1875 to 0.1875
- w_pairout: bfloat16 [128, 128], replicated, may hold values from -0.5 to 0.5
- w_up: bfloat16 [128, 512], replicated, may hold values from -0.5 to 0.5
- w_down: bfloat16 [512, 128], replicated, may hold values from -0.25 to 0.25
Outputs:
- single_out: bfloat16 [512, 1024], P('rows')
- pair_out: bfloat16 [512, 512, 128], P('rows', 'cols')
The draws below stay inside these ranges and needn't reach their ends.
Inputs may be any that keep to these rules, and one draw needn't show every extreme that they name: residue_mask is 1 on a leading run of at least 256 positions and 0 after it.
All inputs are finite; a program needn't handle non-finite values.
Results may differ from the reference program's by a relative error of at most 0.01.
The reference program's roundings to bfloat16 on the way count: a program that leaves them out, or rounds other values in their place, can miss the bound.
Values may be sent and summed in bfloat16 or wider, within the bound.
A program may use at most 64 MiB of HBM per device.

```python
import math
import jax
import jax.numpy as jnp
from jax import lax

SINGLE = 1024
HEADS = 32
HEAD_DIM = 32
PAIR = 128
PAIR_HID = 512
OPD = 64
RESIDUES = 512


def draw_residue_mask(key, part):
    length_now = jax.random.randint(jax.random.fold_in(key, 11), (), RESIDUES // 2, RESIDUES + 1)
    return (jnp.arange(RESIDUES, dtype=jnp.int32) < length_now).astype(jnp.int32)


def draw_w_bias(key, part):
    drawn = jax.random.normal(jax.random.fold_in(key, 23), (PAIR, HEADS), jnp.float32) / jnp.sqrt(jnp.float32(PAIR))
    return jnp.clip(drawn, -40.0, 40.0).astype(jnp.bfloat16)


def block_levels(key, shape, split, smallest, high):
    gain, own = 1.0, jax.random.fold_in(key, 6)
    for position, blocks in split:
        steps = jnp.exp(jax.random.uniform(jax.random.fold_in(own, position), (blocks,), jnp.float32, smallest / len(split), high / len(split)))
        gain = gain * jnp.repeat(steps, shape[position] // blocks).reshape([-1 if axis == position else 1 for axis in range(len(shape))])
    return gain


def scatter_about(stream_key, dims, deviation, limit, split=(), kind=jnp.bfloat16):
    entries = deviation * jax.random.normal(stream_key, dims, jnp.float32)
    if split:
        entries = entries * block_levels(stream_key, dims, split, -0.22, 0.18)
    return jnp.clip(entries, -limit, limit).astype(kind)


def setup_inputs(seed: int = 0) -> dict:
    streams_of = jax.random.split(jax.random.key(seed), 11)
    return {
        "single": scatter_about(streams_of[0], (RESIDUES, SINGLE), 1.0, 6.0, ((0, 4),)),
        "pair": scatter_about(streams_of[1], (RESIDUES, RESIDUES, PAIR), 1.0, 6.0, ((0, 4), (1, 8))),
        "residue_mask": draw_residue_mask(jax.random.fold_in(streams_of[10], 71), 0),
        "w_bias": draw_w_bias(jax.random.fold_in(streams_of[10], 71), 0),
        "w_project": scatter_about(streams_of[4], (4, SINGLE, SINGLE), SINGLE ** -0.5, 0.1875, ((2, 8),)),
        "w_out": scatter_about(streams_of[5], (SINGLE, SINGLE), SINGLE ** -0.5, 0.1875),
        "w_factors": scatter_about(streams_of[6], (SINGLE, 2 * OPD), SINGLE ** -0.5, 0.1875),
        "w_pairout": scatter_about(streams_of[7], (2 * OPD, PAIR), (2 * OPD) ** -0.5, 0.5),
        "w_up": scatter_about(streams_of[8], (PAIR, PAIR_HID), PAIR ** -0.5, 0.5),
        "w_down": scatter_about(streams_of[9], (PAIR_HID, PAIR), PAIR_HID ** -0.5, 0.25),
    }


epsilon = 1e-05

def normalize(values):
    values = values.astype(jnp.float32)
    centred = values - lax.optimization_barrier(jnp.mean(values, -1, keepdims=True))
    return centred * lax.rsqrt(lax.optimization_barrier(jnp.mean(centred * centred, -1, keepdims=True)) + epsilon)

def reference(single, pair, residue_mask, w_bias, w_project, w_out, w_factors, w_pairout, w_up, w_down):
    block_rows = math.gcd(RESIDUES, 32)
    count_blocks = RESIDUES // block_rows
    pair_blocks = pair.reshape(count_blocks, block_rows, RESIDUES, PAIR)

    def bias_block(pair_block):
        normed_pair = normalize(pair_block).astype(jnp.bfloat16)
        return jnp.einsum('rcp,ph->hrc', normed_pair.astype(jnp.float32), w_bias.astype(jnp.float32)).astype(jnp.bfloat16)
    bias_parts = lax.map(bias_block, pair_blocks)
    bias_all = jnp.transpose(bias_parts, (1, 0, 2, 3)).reshape(HEADS, RESIDUES, RESIDUES)
    normed_single = normalize(single).astype(jnp.bfloat16)
    projected = jnp.einsum('rs,fsc->frc', normed_single.astype(jnp.float32), w_project.astype(jnp.float32))
    query_rows = projected[0].astype(jnp.bfloat16).reshape(RESIDUES, HEADS, HEAD_DIM).transpose(1, 0, 2)
    key_rows = projected[1].astype(jnp.bfloat16).reshape(RESIDUES, HEADS, HEAD_DIM).transpose(1, 0, 2)
    value_rows = projected[2].astype(jnp.bfloat16).reshape(RESIDUES, HEADS, HEAD_DIM).transpose(1, 0, 2)
    gate_values = jax.nn.sigmoid(projected[3])
    key_valid = (residue_mask > 0)[None, :]
    score_scale = 1.0 / math.sqrt(HEAD_DIM)

    def attend_head(operands):
        query_head, key_head, value_head, bias_head = operands
        scores = jnp.dot(query_head, key_head.T, preferred_element_type=jnp.float32) * score_scale + bias_head.astype(jnp.float32)
        scores = jnp.where(key_valid, scores, -jnp.inf)
        weights = jax.nn.softmax(scores, axis=-1).astype(jnp.bfloat16)
        return jnp.dot(weights, value_head, preferred_element_type=jnp.float32)
    attended = lax.map(attend_head, (query_rows, key_rows, value_rows, bias_all))
    attended = attended.transpose(1, 0, 2).reshape(RESIDUES, SINGLE)
    mixed = (attended * gate_values).astype(jnp.bfloat16)
    single_out = (single.astype(jnp.float32) + jnp.dot(mixed, w_out, preferred_element_type=jnp.float32)).astype(jnp.bfloat16)
    normed_out = normalize(single_out).astype(jnp.bfloat16)
    factors = jnp.dot(normed_out, w_factors, preferred_element_type=jnp.float32).astype(jnp.bfloat16)
    left_factor = factors[:, :OPD]
    right_factor = factors[:, OPD:]

    def update_block(operands):
        pair_block, left_block = operands
        left_wide = left_block.astype(jnp.float32)[:, None, :]
        right_wide = right_factor.astype(jnp.float32)[None, :, :]
        paired = jnp.concatenate([left_wide * right_wide, left_wide - right_wide], -1).astype(jnp.bfloat16)
        pair_mid = (pair_block.astype(jnp.float32) + jnp.einsum('rcq,qp->rcp', paired.astype(jnp.float32), w_pairout.astype(jnp.float32))).astype(jnp.bfloat16)
        normed_mid = normalize(pair_mid).astype(jnp.bfloat16)
        hidden = jax.nn.relu(jnp.einsum('rcp,pk->rck', normed_mid.astype(jnp.float32), w_up.astype(jnp.float32))).astype(jnp.bfloat16)
        return (pair_mid.astype(jnp.float32) + jnp.einsum('rck,kp->rcp', hidden.astype(jnp.float32), w_down.astype(jnp.float32))).astype(jnp.bfloat16)
    updated = lax.map(update_block, (pair_blocks, left_factor.reshape(count_blocks, block_rows, OPD)))
    return (single_out, updated.reshape(RESIDUES, RESIDUES, PAIR))
```

```python
import functools
import math

import jax
import jax.numpy as jnp
from jax import lax
from jax.experimental import pallas as pl
from jax.experimental.pallas import tpu as pltpu
from jax.sharding import PartitionSpec as P

epsilon = 1e-05


def enter(axes):
    barrier = pltpu.get_barrier_semaphore()
    total = 0
    for axis, size in axes:
        me = lax.axis_index(axis)
        for step in range(1, size):
            pl.semaphore_signal(
                barrier,
                inc=1,
                device_id={axis: lax.rem(me + step, size)},
                device_id_type=pl.DeviceIdType.MESH,
            )
        total += size - 1
    pl.semaphore_wait(barrier, total)


def spread(axis, size, source, landing, send_sems, recv_sems):
    me = lax.axis_index(axis)
    copies = []
    for step in range(1, size):
        copy = pltpu.make_async_remote_copy(
            src_ref=source,
            dst_ref=landing.at[me],
            send_sem=send_sems.at[step - 1],
            recv_sem=recv_sems.at[step - 1],
            device_id={axis: lax.rem(me + step, size)},
            device_id_type=pl.DeviceIdType.MESH,
        )
        copy.start()
        copies.append(copy)
    return copies


def gather_kernel(axis, size, source, gathered, send_sems, recv_sems, own_sem):
    enter([(axis, size)])
    copies = spread(axis, size, source, gathered, send_sems, recv_sems)
    own = pltpu.make_async_copy(source, gathered.at[lax.axis_index(axis)], own_sem)
    own.start()
    own.wait()
    for copy in copies:
        copy.wait()


def gather(values, axis, size, collective_id):
    return pl.pallas_call(
        functools.partial(gather_kernel, axis, size),
        out_shape=jax.ShapeDtypeStruct((size, *values.shape), values.dtype),
        in_specs=[pl.BlockSpec(memory_space=pltpu.VMEM)],
        out_specs=pl.BlockSpec(memory_space=pltpu.VMEM),
        scratch_shapes=[
            pltpu.SemaphoreType.DMA((size - 1,)),
            pltpu.SemaphoreType.DMA((size - 1,)),
            pltpu.SemaphoreType.DMA,
        ],
        compiler_params=pltpu.CompilerParams(collective_id=collective_id, has_side_effects=True),
        name="gather_" + axis,
    )(values)


def single_kernel(
    row_size, col_size, tile_cols,
    mixed, single, w_out, w_factors, single_out, left_out, right_out,
    gathered, factor_right, send_sems, recv_sems, row_send, row_recv, own_sem,
):
    enter([("cols", col_size), ("rows", row_size)])
    tile_rows, width = mixed.shape
    me_col = lax.axis_index("cols")
    me_row = lax.axis_index("rows")
    copies = spread("cols", col_size, mixed, gathered, send_sems, recv_sems)
    own = pltpu.make_async_copy(mixed, gathered.at[me_col], own_sem)
    own.start()
    own.wait()
    for copy in copies:
        copy.wait()
    whole = jnp.concatenate([gathered[part] for part in range(col_size)], axis=1)
    total = jnp.dot(whole, w_out[...], preferred_element_type=jnp.float32)
    updated = (single[...].astype(jnp.float32) + total).astype(jnp.bfloat16)
    single_out[...] = updated
    normed = layer_norm(updated).astype(jnp.bfloat16)
    factors = jnp.dot(normed, w_factors[...], preferred_element_type=jnp.float32)
    factors = factors.astype(jnp.bfloat16).astype(jnp.float32)
    half = factors.shape[1] // 2
    swapped = jnp.concatenate([factors[:, half:], factors[:, :half]], axis=1)
    lower = lax.broadcasted_iota(jnp.int32, factors.shape, 1) < half
    left_out[...] = jnp.where(lower, factors, swapped)
    factor_right[...] = jnp.where(lower, swapped, factors).astype(jnp.bfloat16)
    first = me_col * tile_cols
    owner = first // tile_rows
    offset = pl.multiple_of(first - owner * tile_rows, tile_cols)
    piece = factor_right.at[pl.ds(offset, tile_cols)]

    @pl.when(me_row == owner)
    def _():
        local = pltpu.make_async_copy(piece, right_out, own_sem)
        local.start()
        sends = []
        for step in range(1, row_size):
            send = pltpu.make_async_remote_copy(
                src_ref=piece,
                dst_ref=right_out,
                send_sem=row_send.at[step - 1],
                recv_sem=row_recv,
                device_id={"rows": lax.rem(me_row + step, row_size)},
                device_id_type=pl.DeviceIdType.MESH,
            )
            send.start()
            sends.append(send)
        local.wait()
        for send in sends:
            send.wait_send()

    @pl.when(me_row != owner)
    def _():
        pltpu.make_async_remote_copy(
            src_ref=piece,
            dst_ref=right_out,
            send_sem=row_send.at[0],
            recv_sem=row_recv,
            device_id={"rows": lax.rem(me_row + 1, row_size)},
            device_id_type=pl.DeviceIdType.MESH,
        ).wait_recv()


def update_single(mixed, single, w_out, w_factors, row_size, col_size, tile_cols):
    tile_rows, width = single.shape
    wide = w_factors.shape[1]
    return pl.pallas_call(
        functools.partial(single_kernel, row_size, col_size, tile_cols),
        out_shape=(
            jax.ShapeDtypeStruct((tile_rows, width), jnp.bfloat16),
            jax.ShapeDtypeStruct((tile_rows, wide), jnp.float32),
            jax.ShapeDtypeStruct((tile_cols, wide), jnp.bfloat16),
        ),
        in_specs=[pl.BlockSpec(memory_space=pltpu.VMEM)] * 4,
        out_specs=[pl.BlockSpec(memory_space=pltpu.VMEM)] * 3,
        scratch_shapes=[
            pltpu.VMEM((col_size, *mixed.shape), jnp.bfloat16),
            pltpu.VMEM((tile_rows, wide), jnp.bfloat16),
            pltpu.SemaphoreType.DMA((col_size - 1,)),
            pltpu.SemaphoreType.DMA((col_size - 1,)),
            pltpu.SemaphoreType.DMA((row_size - 1,)),
            pltpu.SemaphoreType.DMA,
            pltpu.SemaphoreType.DMA,
        ],
        compiler_params=pltpu.CompilerParams(collective_id=2, has_side_effects=True),
        name="update_single",
    )(mixed, single, w_out, w_factors)


def norm_kernel(values, normed):
    normed[...] = layer_norm(values[...]).astype(jnp.bfloat16)


def norm_rows(values, block):
    spec = pl.BlockSpec((block, values.shape[1]), lambda step: (step, 0))
    return pl.pallas_call(
        norm_kernel,
        out_shape=jax.ShapeDtypeStruct(values.shape, jnp.bfloat16),
        grid=(values.shape[0] // block,),
        in_specs=[spec],
        out_specs=spec,
        name="norm_pair",
    )(values)


def pair_kernel(pair, left, right, w_pairout, w_up, w_down, updated):
    block_rows, tile_cols, wide = pair.shape
    left_wide = left[...][:, None, :]
    right_wide = right[...].astype(jnp.float32)[None, :, :]
    lower = lax.broadcasted_iota(jnp.int32, pair.shape, 2) < wide // 2
    paired = jnp.where(lower, left_wide * right_wide, left_wide - right_wide)
    paired = paired.astype(jnp.bfloat16).reshape(block_rows * tile_cols, wide)
    flat = pair[...].reshape(block_rows * tile_cols, wide).astype(jnp.float32)
    mid = flat + jnp.dot(paired, w_pairout[...], preferred_element_type=jnp.float32)
    mid = mid.astype(jnp.bfloat16)
    normed = layer_norm(mid).astype(jnp.bfloat16)
    hidden = jnp.dot(normed, w_up[...], preferred_element_type=jnp.float32)
    hidden = jnp.maximum(hidden, 0.0).astype(jnp.bfloat16)
    out = mid.astype(jnp.float32) + jnp.dot(
        hidden, w_down[...], preferred_element_type=jnp.float32
    )
    updated[...] = out.astype(jnp.bfloat16).reshape(pair.shape)


def update_pair(pair, left, right, w_pairout, w_up, w_down):
    tile_rows, tile_cols, wide = pair.shape
    block = math.gcd(tile_rows, max(8, 1024 // tile_cols))
    tile = pl.BlockSpec((block, tile_cols, wide), lambda step: (step, 0, 0))

    def whole(array):
        return pl.BlockSpec(array.shape, lambda step: (0, 0))

    return pl.pallas_call(
        pair_kernel,
        out_shape=jax.ShapeDtypeStruct(pair.shape, jnp.bfloat16),
        grid=(tile_rows // block,),
        in_specs=[
            tile,
            pl.BlockSpec((block, wide), lambda step: (step, 0)),
            whole(right),
            whole(w_pairout),
            whole(w_up),
            whole(w_down),
        ],
        out_specs=tile,
        name="update_pair",
    )(pair, left, right, w_pairout, w_up, w_down)


def layer_norm(values):
    values = values.astype(jnp.float32)
    centred = values - jnp.mean(values, -1, keepdims=True)
    return centred * lax.rsqrt(jnp.mean(centred * centred, -1, keepdims=True) + epsilon)


def per_device(
    row_size, col_size,
    single, pair, residue_mask, w_bias, w_project, w_out, w_factors, w_pairout, w_up, w_down
):
    tile_rows = pair.shape[0]
    tile_cols = pair.shape[1]
    normed_pair = norm_rows(
        pair.reshape(tile_rows * tile_cols, pair.shape[2]), math.gcd(tile_rows * tile_cols, 1024)
    ).reshape(pair.shape)
    bias_local = jnp.einsum(
        "rcp,ph->hrc", normed_pair, w_bias, preferred_element_type=jnp.float32
    ).astype(jnp.bfloat16)
    normed_single = layer_norm(single).astype(jnp.bfloat16)
    projected = jnp.einsum(
        "rs,fsc->frc", normed_single, w_project, preferred_element_type=jnp.float32
    )
    query_rows = projected[0].astype(jnp.bfloat16)
    key_local = projected[1].astype(jnp.bfloat16)
    value_local = projected[2].astype(jnp.bfloat16)
    gate_values = jax.nn.sigmoid(projected[3])
    bias_heads = lax.all_to_all(bias_local, "cols", split_axis=0, concat_axis=2, tiled=True)
    both = gather(jnp.concatenate([key_local, value_local], 1), "rows", row_size, 1)
    both = both.reshape(row_size * tile_rows, both.shape[2])
    key_rows, value_rows = both[:, : key_local.shape[1]], both[:, key_local.shape[1] :]
    heads_here = bias_heads.shape[0]
    head_width = query_rows.shape[1] // heads_here
    residues = key_rows.shape[0]
    query_split = query_rows.reshape(tile_rows, heads_here, head_width)
    key_split = key_rows.reshape(residues, heads_here, head_width)
    value_split = value_rows.reshape(residues, heads_here, head_width)
    score_scale = 1.0 / math.sqrt(head_width)
    scores = jnp.einsum(
        "rhd,lhd->hrl", query_split, key_split, preferred_element_type=jnp.float32
    ) * score_scale + bias_heads.astype(jnp.float32)
    key_valid = (residue_mask > 0)[None, None, :]
    scores = jnp.where(key_valid, scores, -jnp.inf)
    weights = jax.nn.softmax(scores, axis=-1).astype(jnp.bfloat16)
    attended = jnp.einsum("hrl,lhd->rhd", weights, value_split, preferred_element_type=jnp.float32)
    attended = attended.reshape(tile_rows, heads_here * head_width)
    mixed = (attended * gate_values).astype(jnp.bfloat16)
    single_out, left, right = update_single(
        mixed, single, w_out, w_factors, row_size, col_size, tile_cols
    )
    return (single_out, update_pair(pair, left, right, w_pairout, w_up, w_down))


def solution(mesh):
    return jax.shard_map(
        functools.partial(per_device, mesh.shape["rows"], mesh.shape["cols"]),
        mesh=mesh,
        in_specs=(
            P("rows", None),
            P("rows", "cols", None),
            P(),
            P(),
            P(None, None, "cols"),
            P(),
            P(),
            P(),
            P(),
            P(),
        ),
        out_specs=(P("rows", None), P("rows", "cols", None)),
        check_vma=False,
    )
```

```python
import functools
import math

import jax
import jax.numpy as jnp
from jax import lax
from jax.experimental import pallas as pl
from jax.experimental.pallas import tpu as pltpu
from jax.sharding import PartitionSpec as P

epsilon = 1e-05


def enter(axes):
    barrier = pltpu.get_barrier_semaphore()
    total = 0
    for axis, size in axes:
        me = lax.axis_index(axis)
        for step in range(1, size):
            pl.semaphore_signal(
                barrier,
                inc=1,
                device_id={axis: lax.rem(me + step, size)},
                device_id_type=pl.DeviceIdType.MESH,
            )
        total += size - 1
    pl.semaphore_wait(barrier, total)


def spread(axis, size, source, landing, send_sems, recv_sems):
    me = lax.axis_index(axis)
    copies = []
    for step in range(1, size):
        copy = pltpu.make_async_remote_copy(
            src_ref=source,
            dst_ref=landing.at[me],
            send_sem=send_sems.at[step - 1],
            recv_sem=recv_sems.at[step - 1],
            device_id={axis: lax.rem(me + step, size)},
            device_id_type=pl.DeviceIdType.MESH,
        )
        copy.start()
        copies.append(copy)
    return copies


def gather_kernel(axis, size, source, gathered, send_sems, recv_sems, own_sem):
    enter([(axis, size)])
    copies = spread(axis, size, source, gathered, send_sems, recv_sems)
    own = pltpu.make_async_copy(source, gathered.at[lax.axis_index(axis)], own_sem)
    own.start()
    own.wait()
    for copy in copies:
        copy.wait()


def gather(values, axis, size, collective_id):
    return pl.pallas_call(
        functools.partial(gather_kernel, axis, size),
        out_shape=jax.ShapeDtypeStruct((size, *values.shape), values.dtype),
        in_specs=[pl.BlockSpec(memory_space=pltpu.VMEM)],
        out_specs=pl.BlockSpec(memory_space=pltpu.VMEM),
        scratch_shapes=[
            pltpu.SemaphoreType.DMA((size - 1,)),
            pltpu.SemaphoreType.DMA((size - 1,)),
            pltpu.SemaphoreType.DMA,
        ],
        compiler_params=pltpu.CompilerParams(collective_id=collective_id, has_side_effects=True),
        name="gather_" + axis,
    )(values)


def single_kernel(
    row_size, col_size, tile_cols,
    mixed, single, w_out, w_factors, single_out, left_out, right_out,
    gathered, factor_right, send_sems, recv_sems, row_send, row_recv, own_sem,
):
    enter([("cols", col_size), ("rows", row_size)])
    tile_rows, width = mixed.shape
    me_col = lax.axis_index("cols")
    me_row = lax.axis_index("rows")
    copies = spread("cols", col_size, mixed, gathered, send_sems, recv_sems)
    own = pltpu.make_async_copy(mixed, gathered.at[me_col], own_sem)
    own.start()
    own.wait()
    for copy in copies:
        copy.wait()
    whole = jnp.concatenate([gathered[part] for part in range(col_size)], axis=1)
    total = jnp.dot(whole, w_out[...], preferred_element_type=jnp.float32)
    updated = (single[...].astype(jnp.float32) + total).astype(jnp.bfloat16)
    single_out[...] = updated
    normed = layer_norm(updated).astype(jnp.bfloat16)
    factors = jnp.dot(normed, w_factors[...], preferred_element_type=jnp.float32)
    factors = factors.astype(jnp.bfloat16).astype(jnp.float32)
    half = factors.shape[1] // 2
    swapped = jnp.concatenate([factors[:, half:], factors[:, :half]], axis=1)
    lower = lax.broadcasted_iota(jnp.int32, factors.shape, 1) < half
    left_out[...] = jnp.where(lower, factors, swapped)
    factor_right[...] = jnp.where(lower, swapped, factors).astype(jnp.bfloat16)
    first = me_col * tile_cols
    owner = first // tile_rows
    offset = pl.multiple_of(first - owner * tile_rows, tile_cols)
    piece = factor_right.at[pl.ds(offset, tile_cols)]

    @pl.when(me_row == owner)
    def _():
        local = pltpu.make_async_copy(piece, right_out, own_sem)
        local.start()
        sends = []
        for step in range(1, row_size):
            send = pltpu.make_async_remote_copy(
                src_ref=piece,
                dst_ref=right_out,
                send_sem=row_send.at[step - 1],
                recv_sem=row_recv,
                device_id={"rows": lax.rem(me_row + step, row_size)},
                device_id_type=pl.DeviceIdType.MESH,
            )
            send.start()
            sends.append(send)
        local.wait()
        for send in sends:
            send.wait_send()

    @pl.when(me_row != owner)
    def _():
        pltpu.make_async_remote_copy(
            src_ref=piece,
            dst_ref=right_out,
            send_sem=row_send.at[0],
            recv_sem=row_recv,
            device_id={"rows": lax.rem(me_row + 1, row_size)},
            device_id_type=pl.DeviceIdType.MESH,
        ).wait_recv()


def update_single(mixed, single, w_out, w_factors, row_size, col_size, tile_cols):
    tile_rows, width = single.shape
    wide = w_factors.shape[1]
    return pl.pallas_call(
        functools.partial(single_kernel, row_size, col_size, tile_cols),
        out_shape=(
            jax.ShapeDtypeStruct((tile_rows, width), jnp.bfloat16),
            jax.ShapeDtypeStruct((tile_rows, wide), jnp.float32),
            jax.ShapeDtypeStruct((tile_cols, wide), jnp.bfloat16),
        ),
        in_specs=[pl.BlockSpec(memory_space=pltpu.VMEM)] * 4,
        out_specs=[pl.BlockSpec(memory_space=pltpu.VMEM)] * 3,
        scratch_shapes=[
            pltpu.VMEM((col_size, *mixed.shape), jnp.bfloat16),
            pltpu.VMEM((tile_rows, wide), jnp.bfloat16),
            pltpu.SemaphoreType.DMA((col_size - 1,)),
            pltpu.SemaphoreType.DMA((col_size - 1,)),
            pltpu.SemaphoreType.DMA((row_size - 1,)),
            pltpu.SemaphoreType.DMA,
            pltpu.SemaphoreType.DMA,
        ],
        compiler_params=pltpu.CompilerParams(collective_id=2, has_side_effects=True),
        name="update_single",
    )(mixed, single, w_out, w_factors)


def matmul_norm(values):
    wide = values.shape[1]
    share = jnp.full((2 * wide, wide), 1.0 / wide, jnp.bfloat16)
    mean = jnp.dot(values, share[:wide], preferred_element_type=jnp.float32)
    centred = values.astype(jnp.float32) - mean
    square = centred * centred
    high = square.astype(jnp.bfloat16)
    low = (square - high.astype(jnp.float32)).astype(jnp.bfloat16)
    spread_out = jnp.dot(
        jnp.concatenate([high, low], 1), share, preferred_element_type=jnp.float32
    )
    return (centred * lax.rsqrt(spread_out + epsilon)).astype(jnp.bfloat16)


def norm_kernel(values, normed):
    normed[...] = matmul_norm(values[...])


def norm_rows(values, block):
    spec = pl.BlockSpec((block, values.shape[1]), lambda step: (step, 0))
    return pl.pallas_call(
        norm_kernel,
        out_shape=jax.ShapeDtypeStruct(values.shape, jnp.bfloat16),
        grid=(values.shape[0] // block,),
        in_specs=[spec],
        out_specs=spec,
        name="norm_pair",
    )(values)


def pair_kernel(pair, left, right, w_pairout, w_up, w_down, updated):
    block_rows, tile_cols, wide = pair.shape
    left_wide = left[...][:, None, :]
    right_wide = right[...].astype(jnp.float32)[None, :, :]
    lower = lax.broadcasted_iota(jnp.int32, pair.shape, 2) < wide // 2
    paired = jnp.where(lower, left_wide * right_wide, left_wide - right_wide)
    paired = paired.astype(jnp.bfloat16).reshape(block_rows * tile_cols, wide)
    flat = pair[...].reshape(block_rows * tile_cols, wide).astype(jnp.float32)
    mid = flat + jnp.dot(paired, w_pairout[...], preferred_element_type=jnp.float32)
    mid = mid.astype(jnp.bfloat16)
    normed = matmul_norm(mid)
    hidden = jnp.dot(normed, w_up[...], preferred_element_type=jnp.float32)
    hidden = jnp.maximum(hidden, 0.0).astype(jnp.bfloat16)
    out = mid.astype(jnp.float32) + jnp.dot(
        hidden, w_down[...], preferred_element_type=jnp.float32
    )
    updated[...] = out.astype(jnp.bfloat16).reshape(pair.shape)


def update_pair(pair, left, right, w_pairout, w_up, w_down):
    tile_rows, tile_cols, wide = pair.shape
    block = math.gcd(tile_rows, max(8, 1024 // tile_cols))
    tile = pl.BlockSpec((block, tile_cols, wide), lambda step: (step, 0, 0))

    def whole(array):
        return pl.BlockSpec(array.shape, lambda step: (0, 0))

    return pl.pallas_call(
        pair_kernel,
        out_shape=jax.ShapeDtypeStruct(pair.shape, jnp.bfloat16),
        grid=(tile_rows // block,),
        in_specs=[
            tile,
            pl.BlockSpec((block, wide), lambda step: (step, 0)),
            whole(right),
            whole(w_pairout),
            whole(w_up),
            whole(w_down),
        ],
        out_specs=tile,
        name="update_pair",
    )(pair, left, right, w_pairout, w_up, w_down)


def layer_norm(values):
    values = values.astype(jnp.float32)
    centred = values - jnp.mean(values, -1, keepdims=True)
    return centred * lax.rsqrt(jnp.mean(centred * centred, -1, keepdims=True) + epsilon)


def per_device(
    row_size, col_size,
    single, pair, residue_mask, w_bias, w_project, w_out, w_factors, w_pairout, w_up, w_down
):
    tile_rows = pair.shape[0]
    tile_cols = pair.shape[1]
    normed_pair = norm_rows(
        pair.reshape(tile_rows * tile_cols, pair.shape[2]), math.gcd(tile_rows * tile_cols, 1024)
    ).reshape(pair.shape)
    bias_local = jnp.einsum(
        "rcp,ph->hrc", normed_pair, w_bias, preferred_element_type=jnp.float32
    ).astype(jnp.bfloat16)
    normed_single = layer_norm(single).astype(jnp.bfloat16)
    projected = jnp.einsum(
        "rs,fsc->frc", normed_single, w_project, preferred_element_type=jnp.float32
    )
    query_rows = projected[0].astype(jnp.bfloat16)
    key_local = projected[1].astype(jnp.bfloat16)
    value_local = projected[2].astype(jnp.bfloat16)
    gate_values = jax.nn.sigmoid(projected[3])
    bias_heads = lax.all_to_all(bias_local, "cols", split_axis=0, concat_axis=2, tiled=True)
    both = gather(jnp.concatenate([key_local, value_local], 1), "rows", row_size, 1)
    both = both.reshape(row_size * tile_rows, both.shape[2])
    key_rows, value_rows = both[:, : key_local.shape[1]], both[:, key_local.shape[1] :]
    heads_here = bias_heads.shape[0]
    head_width = query_rows.shape[1] // heads_here
    residues = key_rows.shape[0]
    query_split = query_rows.reshape(tile_rows, heads_here, head_width)
    key_split = key_rows.reshape(residues, heads_here, head_width)
    value_split = value_rows.reshape(residues, heads_here, head_width)
    score_scale = 1.0 / math.sqrt(head_width)
    scores = jnp.einsum(
        "rhd,lhd->hrl", query_split, key_split, preferred_element_type=jnp.float32
    ) * score_scale + bias_heads.astype(jnp.float32)
    key_valid = (residue_mask > 0)[None, None, :]
    scores = jnp.where(key_valid, scores, -jnp.inf)
    weights = jax.nn.softmax(scores, axis=-1).astype(jnp.bfloat16)
    attended = jnp.einsum("hrl,lhd->rhd", weights, value_split, preferred_element_type=jnp.float32)
    attended = attended.reshape(tile_rows, heads_here * head_width)
    mixed = (attended * gate_values).astype(jnp.bfloat16)
    single_out, left, right = update_single(
        mixed, single, w_out, w_factors, row_size, col_size, tile_cols
    )
    return (single_out, update_pair(pair, left, right, w_pairout, w_up, w_down))


def solution(mesh):
    return jax.shard_map(
        functools.partial(per_device, mesh.shape["rows"], mesh.shape["cols"]),
        mesh=mesh,
        in_specs=(
            P("rows", None),
            P("rows", "cols", None),
            P(),
            P(),
            P(None, None, "cols"),
            P(),
            P(),
            P(),
            P(),
            P(),
        ),
        out_specs=(P("rows", None), P("rows", "cols", None)),
        check_vma=False,
    )
```
